32 devices in a mesh: dp: 4 (over z), win: 2 (over y), mp: 4 (over x, core).
Axes of the slice: x: 2, y: 2, z: 4, core: 2. Of those that a mesh axis runs over, the one named last changes fastest.
Arguments:
- tokens: bfloat16 [9408, 768], P(('dp', 'win', 'mp')), may hold values from -6 to 6
- target: bfloat16 [9408, 768], P(('dp', 'win', 'mp')), may hold values from -16 to 16
- regions: int32 [192, 49], P(('dp', 'win')), may hold values from 0 to 3
- rel_index: int32 [49, 49], replicated, may hold values from 0 to 168
- layer_norm_gain: float32 [768], replicated, may hold values from 0.5 to 1.5
- bias_table: float32 [169, 24], P(None, 'mp'), may hold values from -5 to 330
- w_qkv: bfloat16 [3, 768, 768], P(None, 'mp'), may hold values from -0.21875 to 0.21875
- w_proj: bfloat16 [768, 768], P('mp'), may hold values from -0.21875 to 0.21875
Outputs:
- input_gradient: float32 [9408, 768], P(('dp', 'win', 'mp'))
- grad_qkv: float32 [3, 768, 768], P(None, 'mp', ('dp', 'win'))
- grad_proj: float32 [768, 768], P('mp', ('dp', 'win'))
- grad_table: float32 [169, 24], P(None, 'mp')
- gain_gradient: float32 [768], replicated
- loss: float32 [], replicated
The draws below stay inside these ranges and needn't reach their ends.
All inputs are finite; a program needn't handle non-finite values.
Results may differ from the reference program's by a relative error of at most 0.01.
Values may be sent and summed in bfloat16 or wider, within the bound.
No kernel may reach another device: no remote copies, remote signals or barrier semaphores. Data moves between devices by JAX's collectives and lax.ppermute only.
A program may use at most 64 MiB of HBM per device.

```python
import jax
import jax.numpy as jnp
from jax import lax

C = 768
HEADS = 24
HD = 32
WIN_TOK = 49
TABLE = 169
WINDOWS = 192
TOKENS = 9408
N_MP = 4


def draw_bias_table(key, part):
    base_key = jax.random.fold_in(jax.random.fold_in(key, 7), 0)
    base = jnp.clip(jax.random.normal(base_key, (TABLE, HEADS), jnp.float32), -5.0, 5.0)
    return base


def draw_target(key, part):
    noise_key = jax.random.fold_in(key, 11)
    fraction = jnp.arange(TOKENS, dtype=jnp.float32)[:, None] / (TOKENS - 1.0)
    noise = jnp.clip(jax.random.normal(noise_key, (TOKENS, C), jnp.float32), -4.0, 4.0)
    result = noise * (1.0 + 3.0 * fraction)
    return result.astype(jnp.bfloat16)


def touch_ends(values, rng, smallest, largest):
    place = [jax.random.randint(jax.random.fold_in(rng, axis), (), 0, length) for axis, length in enumerate(values.shape)]
    main_axis = values.shape.index(max(values.shape))
    next_to = place[:main_axis] + [(place[main_axis] + 1) % values.shape[main_axis]] + place[main_axis + 1:]
    return values.at[tuple(place)].set(smallest).at[tuple(next_to)].set(largest)


def level_of(own_key, extent, pieces, low, high):
    gain = 1.0
    for position, shards_of in pieces:
        draws = jax.random.uniform(jax.random.fold_in(jax.random.fold_in(own_key, 6), position), (shards_of,), jnp.float32, low / len(pieces), high / len(pieces))
        gain = gain * jnp.repeat(jnp.exp(draws), extent[position] // shards_of).reshape((-1,) + (1,) * (len(extent) - 1 - position))
    return gain


def centred(stream_key, shape, width, most, pieces=(), kind=jnp.bfloat16):
    entries = width * jax.random.normal(stream_key, shape, jnp.float32)
    if pieces:
        entries = entries * level_of(stream_key, shape, pieces, -0.22, 0.18)
    return jnp.clip(entries, -most, most).astype(kind)


def setup_inputs(seed: int = 0) -> dict:
    key_of = jax.random.split(jax.random.key(seed), 9)
    tokens = centred(key_of[0], (TOKENS, C), 1.0, 6.0, ((0, 32),))
    target = draw_target(jax.random.fold_in(key_of[8], 71), 0)
    regions = touch_ends(jax.random.randint(key_of[2], (WINDOWS, WIN_TOK), 0, 4), jax.random.fold_in(key_of[2], 1), 0, 3).astype(jnp.int32)
    rel_index = touch_ends(jax.random.randint(key_of[3], (WIN_TOK, WIN_TOK), 0, TABLE), jax.random.fold_in(key_of[3], 1), 0, TABLE - 1).astype(jnp.int32)
    layer_norm_gain = jnp.clip(1.0 + 0.1 * jax.random.normal(key_of[4], (C,), jnp.float32), 0.5, 1.5)
    bias_table = draw_bias_table(jax.random.fold_in(key_of[8], 71), 0)
    w_qkv = centred(key_of[6], (3, C, C), C ** -0.5, 0.21875, ((1, 4),))
    w_proj = centred(key_of[7], (C, C), C ** -0.5, 0.21875, ((0, 4),))
    return dict(tokens=tokens, target=target, regions=regions, rel_index=rel_index, layer_norm_gain=layer_norm_gain, bias_table=bias_table, w_qkv=w_qkv, w_proj=w_proj)


def group_sum(left, right, form):

    def step(total, pair):
        term = jnp.einsum(form, pair[0].astype(jnp.float32), pair[1].astype(jnp.float32))
        rounded = lax.optimization_barrier(term.astype(jnp.bfloat16))
        return (total + rounded.astype(jnp.float32), None)
    first = jnp.einsum(form, left[0].astype(jnp.float32), right[0].astype(jnp.float32))
    total, unused = lax.scan(step, jnp.zeros(first.shape, jnp.float32), (left, right))
    return total

def reference(tokens, target, regions, rel_index, layer_norm_gain, bias_table, w_qkv, w_proj):
    f32 = jnp.float32
    brain_float_sixteen = jnp.bfloat16
    group_cols = C // N_MP
    x = tokens.astype(f32)
    mean_value = lax.optimization_barrier(jnp.mean(x, axis=1, keepdims=True))
    centered_input = x - mean_value
    var = lax.optimization_barrier(jnp.mean(centered_input * centered_input, axis=1, keepdims=True))
    inverse_deviation = lax.rsqrt(var + 1e-05)
    normalized_input = centered_input * inverse_deviation
    normed_input = (normalized_input * layer_norm_gain[None, :]).astype(brain_float_sixteen)
    qkv = jnp.einsum('rc,thc->trh', normed_input.astype(f32), w_qkv.astype(f32))
    scale = HD ** (-0.5)
    shape4 = (WINDOWS, WIN_TOK, HEADS, HD)
    query = (qkv[0] * scale).astype(brain_float_sixteen).reshape(shape4)
    keys = qkv[1].astype(brain_float_sixteen).reshape(shape4)
    values = qkv[2].astype(brain_float_sixteen).reshape(shape4)
    onehot = (rel_index.reshape(-1)[:, None] == jnp.arange(TABLE, dtype=jnp.int32)[None, :]).astype(f32)
    relbias = jnp.dot(onehot, bias_table, precision=lax.Precision.HIGHEST).T.reshape(HEADS, WIN_TOK, WIN_TOK)
    maskv = jnp.where(regions[:, :, None] == regions[:, None, :], 0.0, -100.0).astype(f32)
    scores = jnp.einsum('wqhd,wkhd->whqk', query.astype(f32), keys.astype(f32))
    scores = scores + relbias[None] + maskv[:, None]
    top = lax.optimization_barrier(jnp.max(scores, axis=-1, keepdims=True))
    expo = jnp.exp(scores - top)
    probs = expo / lax.optimization_barrier(jnp.sum(expo, axis=-1, keepdims=True))
    pb = probs.astype(brain_float_sixteen)
    attn = jnp.einsum('whqk,wkhd->wqhd', pb.astype(f32), values.astype(f32)).astype(brain_float_sixteen).reshape(TOKENS, C)
    attn_groups = attn.reshape(TOKENS, N_MP, group_cols).transpose(1, 0, 2)
    proj_groups = w_proj.reshape(N_MP, group_cols, C)
    ysum = group_sum(attn_groups, proj_groups, 'rh,hc->rc')
    error_values = x + ysum - target.astype(f32)
    loss = 0.5 * jnp.sum(error_values * error_values) / TOKENS
    gb = error_values.astype(brain_float_sixteen)
    dproj = jnp.dot(attn.T, gb, preferred_element_type=f32)
    dattn = jnp.dot(gb, w_proj.T, preferred_element_type=f32).astype(brain_float_sixteen).reshape(shape4)
    dprob = jnp.einsum('wqhd,wkhd->whqk', dattn.astype(f32), values.astype(f32))
    dvalue = jnp.einsum('whqk,wqhd->wkhd', pb.astype(f32), dattn.astype(f32))
    dscore = probs * (dprob - lax.optimization_barrier(jnp.sum(probs * dprob, axis=-1, keepdims=True)))
    dtable = jnp.dot(lax.optimization_barrier(jnp.sum(dscore, axis=0)).reshape(HEADS, -1), onehot, precision=lax.Precision.HIGHEST).T
    dbf = dscore.astype(brain_float_sixteen).astype(f32)
    dquery = jnp.einsum('whqk,wkhd->wqhd', dbf, keys.astype(f32)) * scale
    dkey = jnp.einsum('whqk,wqhd->wkhd', dbf, query.astype(f32))
    dqkv = jnp.stack([dquery, dkey, dvalue]).astype(brain_float_sixteen).reshape(3, TOKENS, C)
    dwqkv = jnp.einsum('trh,rc->thc', dqkv.astype(f32), normed_input.astype(f32))
    dqkv_groups = dqkv.reshape(3, TOKENS, N_MP, group_cols).transpose(2, 0, 1, 3)
    wqkv_groups = w_qkv.reshape(3, N_MP, group_cols, C).transpose(1, 0, 2, 3)
    normed_output_gradient = group_sum(dqkv_groups, wqkv_groups, 'trh,thc->rc')
    normalized_gradient = normed_output_gradient * layer_norm_gain[None, :]
    gradient_mean_first = lax.optimization_barrier(jnp.mean(normalized_gradient, axis=1, keepdims=True))
    gradient_mean_second = lax.optimization_barrier(jnp.mean(normalized_gradient * normalized_input, axis=1, keepdims=True))
    input_gradient = error_values + inverse_deviation * (normalized_gradient - gradient_mean_first - normalized_input * gradient_mean_second)
    shrink_factor = TOKENS ** (-0.5)
    gain_gradient = lax.optimization_barrier(jnp.sum(normed_output_gradient * normalized_input, axis=0)) * shrink_factor
    return (input_gradient, dwqkv * shrink_factor, dproj * shrink_factor, dtable * shrink_factor, gain_gradient, loss)
```

```python
import functools

import jax
import jax.numpy as jnp
from jax import lax
from jax.experimental import pallas as pl
from jax.experimental.pallas import tpu as pltpu
from jax.sharding import PartitionSpec as P

HD = 32
WIN_TOK = 49
TABLE = 169
F32 = jnp.float32
BF16 = jnp.bfloat16
NEG = -1e30


def nt(a, b):
    return lax.dot_general(a, b, (((1,), (1,)), ((), ())), preferred_element_type=F32)


def nn(a, b):
    return lax.dot_general(a, b, (((1,), (0,)), ((), ())), preferred_element_type=F32)


def tn(a, b):
    return lax.dot_general(a, b, (((0,), (0,)), ((), ())), preferred_element_type=F32)


def head_masks(width, dtype):
    lane = lax.broadcasted_iota(jnp.int32, (1, width), 1) // HD
    return [(lane == h).astype(F32).astype(dtype) for h in range(width // HD)]


def stack_heads(a, masks):
    return jnp.concatenate([a * m for m in masks], axis=0)


def fold_heads(a, masks, rows):
    total = a[:rows] * masks[0]
    for h in range(1, len(masks)):
        total = total + a[h * rows : (h + 1) * rows] * masks[h]
    return total


def norm(x):
    width = x.shape[1]
    mean = jnp.sum(x, axis=1, keepdims=True) / width
    centered = x - mean
    var = jnp.sum(centered * centered, axis=1, keepdims=True) / width
    inv = lax.rsqrt(var + 1e-05)
    return centered * inv, inv


def forward_kernel(xa, xb, ma, mb, gain, w, relb, *outs):
    rows = xa.shape[1]
    width = w.shape[1]
    heads = width // HD
    x = jnp.concatenate([xa[0], xb[0]], axis=0).astype(F32)
    xhat, _ = norm(x)
    xn = (xhat * gain[...]).astype(BF16)
    q = (nt(xn, w[0]) * (HD**-0.5)).astype(BF16)
    k = nt(xn, w[1]).astype(BF16)
    v = nt(xn, w[2]).astype(BF16)
    mb16 = head_masks(width, BF16)
    mf32 = head_masks(width, F32)
    for i, mask in enumerate((ma, mb)):
        attn_out, q_out, k_out, v_out, p_out, xn_out = outs[6 * i : 6 * i + 6]
        span = slice(i * rows, (i + 1) * rows)
        qi, ki, vi = q[span], k[span], v[span]
        s = nt(stack_heads(qi, mb16), ki)
        s = (s + relb[...]).reshape(heads, rows, rows) + mask[...]
        s = s.reshape(heads * rows, rows)
        e = jnp.exp(s - jnp.max(s, axis=1, keepdims=True))
        probs = e * (1.0 / jnp.sum(e, axis=1, keepdims=True))
        o = nn(probs.astype(BF16), vi)
        attn_out[0] = fold_heads(o, mf32, rows).astype(BF16)
        q_out[0] = qi
        k_out[0] = ki
        v_out[0] = vi
        p_out[0] = probs
        xn_out[0] = xn[span]


def middle_kernel(count, valid, *refs):
    attns = refs[:count]
    projs = refs[count : 2 * count]
    x, target, gy_out, gb_out, sq_out = refs[2 * count :]
    total = jnp.zeros(x.shape[1:], F32)
    for a, w in zip(attns, projs):
        total = total + nn(a[0], w[...]).astype(BF16).astype(F32)
    gy = x[0].astype(F32) + total - target[0].astype(F32)
    row = lax.broadcasted_iota(jnp.int32, gy.shape, 0)
    gy = jnp.where(row < valid, gy, 0.0)
    gy_out[0] = gy
    gb_out[0] = gy.astype(BF16)

    @pl.when(pl.program_id(0) == 0)
    def _():
        sq_out[...] = jnp.zeros_like(sq_out)

    sq_out[...] += jnp.sum(gy * gy, axis=0, keepdims=True)


def backward_kernel(first, last, factor, *refs):
    ins = (refs[:7], refs[7:14])
    wp, w = refs[14:16]
    refs = refs[16:]
    if not first:
        acc_in, tab_in = refs[:2]
        refs = refs[2:]
    dxa, dxb, acc_out, tab_out = refs[:4]
    acc = refs[4] if last else acc_out
    width = w.shape[1]
    rows = dxa.shape[1]

    @pl.when(pl.program_id(0) == 0)
    def _():
        if first:
            acc[...] = jnp.zeros_like(acc)
            tab_out[...] = jnp.zeros_like(tab_out)
        else:
            acc[...] = acc_in[...]
            tab_out[...] = tab_in[...]

    mb16 = head_masks(width, BF16)
    mf32 = head_masks(width, F32)
    gb = jnp.concatenate([ins[0][0][0], ins[1][0][0]], axis=0)
    attn = jnp.concatenate([ins[0][1][0], ins[1][1][0]], axis=0)
    xn = jnp.concatenate([ins[0][6][0], ins[1][6][0]], axis=0)
    dattn = nt(gb, wp[...]).astype(BF16)
    parts = ([], [], [])
    table = tab_out[...]
    for i in range(2):
        _, _, q, k, v, p, _ = ins[i]
        das = stack_heads(dattn[i * rows : (i + 1) * rows], mb16)
        probs = p[0]
        pb = probs.astype(BF16)
        dprob = nt(das, v[0])
        ds = probs * (dprob - jnp.sum(probs * dprob, axis=1, keepdims=True))
        table = table + ds
        db = ds.astype(BF16)
        dq = fold_heads(nn(db, k[0]), mf32, rows) * (HD**-0.5)
        dk = tn(db, stack_heads(q[0], mb16))
        dv = tn(pb, das)
        for part, value in zip(parts, (dq, dk, dv)):
            part.append(value.astype(BF16))
    tab_out[...] = table
    grads = [jnp.concatenate(part, axis=0) for part in parts]
    dxn = nn(grads[0], w[0]) + nn(grads[1], w[1]) + nn(grads[2], w[2])
    dxa[0] = dxn[:rows].astype(BF16)
    dxb[0] = dxn[rows:].astype(BF16)
    for t in range(3):
        acc[t * width : (t + 1) * width] += tn(grads[t], xn)
    acc[3 * width :] += tn(attn, gb)
    if last:

        @pl.when(pl.program_id(0) == pl.num_programs(0) - 1)
        def _():
            acc_out[...] = (acc[...] * factor).T.astype(BF16)


def final_kernel(count, *refs):
    parts = refs[:count]
    x, gy, gain, out, gg_out = refs[count:]
    width = x.shape[2]
    xhat, inv = norm(x[0].astype(F32))
    dxn = parts[0][0].astype(F32)
    for part in parts[1:]:
        dxn = dxn + part[0].astype(F32)
    dxhat = dxn * gain[...]
    m1 = jnp.sum(dxhat, axis=1, keepdims=True) / width
    m2 = jnp.sum(dxhat * xhat, axis=1, keepdims=True) / width
    out[0] = gy[0] + inv * (dxhat - m1 - xhat * m2)

    @pl.when(pl.program_id(0) == 0)
    def _():
        gg_out[...] = jnp.zeros_like(gg_out)

    gg_out[...] += jnp.sum(dxn * xhat, axis=0, keepdims=True)


def step_spec(*shape):
    return pl.BlockSpec((1,) + shape, lambda p: (p,) + (0,) * len(shape))


def whole_spec(*shape):
    return pl.BlockSpec(shape, lambda p: (0,) * len(shape))


PARAMS = pltpu.CompilerParams(dimension_semantics=("arbitrary",))


def per_device(tokens, target, regions, rel_index, layer_norm_gain, bias_table, w_qkv, w_proj):
    owned_rows, channels = tokens.shape
    width = w_qkv.shape[1]
    heads = width // HD
    mp = lax.axis_size("mp")
    me = lax.axis_index("mp")
    spread = lax.axis_size("dp") * lax.axis_size("win")
    everyone = owned_rows * spread * mp
    factor = everyone ** (-0.5)
    owned_windows = owned_rows // WIN_TOK
    group = 2 if owned_windows % 2 == 0 else 1
    steps = owned_windows // group
    valid = group * WIN_TOK
    rows = -(-valid // 16) * 16
    stacked = heads * rows

    def pack(a):
        a = a.reshape(steps, valid, channels)
        return jnp.pad(a, ((0, 0), (0, rows - valid), (0, 0)))

    def swap(a, k):
        return lax.ppermute(a, "mp", [(i, i ^ k) for i in range(mp)])

    def gather(a, after=None):
        blocks = [a]
        for k in range(1, mp):
            blocks.append(swap(blocks[k - 1], 1) if k % 2 else swap(a, k))
        return blocks

    x = pack(tokens)
    tgt = pack(target)
    xs = gather(x)
    tied, _ = lax.optimization_barrier((w_proj, xs[mp - 2]))
    projs = gather(tied)

    onehot = (rel_index.reshape(-1)[:, None] == jnp.arange(TABLE, dtype=jnp.int32)[None, :]).astype(F32)
    relbias = jnp.dot(onehot, bias_table, precision=lax.Precision.HIGHEST).T.reshape(heads, WIN_TOK, WIN_TOK)
    relb = jnp.zeros((heads, rows, rows), F32)
    for g in range(group):
        lo = g * WIN_TOK
        hi = rows - lo - WIN_TOK
        relb = relb + jnp.pad(relbias, ((0, 0), (lo, hi), (lo, hi)))
    relb = relb.reshape(stacked, rows)

    tags = regions.reshape(mp, steps, valid)
    tags = jnp.pad(tags, ((0, 0), (0, 0), (0, rows - valid)), constant_values=-1)
    spot = jnp.arange(rows, dtype=jnp.int32)
    near = (spot[:, None] // WIN_TOK == spot[None, :] // WIN_TOK) & (spot[None, :] < valid)
    maskv = jnp.where(tags[..., :, None] == tags[..., None, :], 0.0, -100.0)
    maskv = jnp.where(near, maskv, NEG).astype(F32)
    masks = [lax.dynamic_index_in_dim(maskv, me ^ k, 0, keepdims=False) for k in range(mp)]

    gain = layer_norm_gain[None, :]
    block_shapes = ((rows, width), (rows, width), (rows, width), (rows, width), (stacked, rows), (rows, channels))
    block_types = (BF16, BF16, BF16, BF16, F32, BF16)
    forward = pl.pallas_call(
        forward_kernel,
        grid=(steps,),
        in_specs=[step_spec(rows, channels)] * 2
        + [step_spec(rows, rows)] * 2
        + [whole_spec(1, channels), whole_spec(3, width, channels), whole_spec(stacked, rows)],
        out_specs=[step_spec(*s) for s in block_shapes] * 2,
        out_shape=[jax.ShapeDtypeStruct((steps,) + s, t) for s, t in zip(block_shapes, block_types)] * 2,
        compiler_params=PARAMS,
        name="forward",
    )
    saved = []
    for j in range(0, mp, 2):
        res = forward(xs[j], xs[j + 1], masks[j], masks[j + 1], gain, w_qkv, relb)
        saved += [res[:6], res[6:]]

    attns = [saved[0][0]] + [swap(saved[k][0], k) for k in range(1, mp)]
    gy, gb, squares = pl.pallas_call(
        functools.partial(middle_kernel, mp, valid),
        grid=(steps,),
        in_specs=[step_spec(rows, width)] * mp
        + [whole_spec(width, channels)] * mp
        + [step_spec(rows, channels)] * 2,
        out_specs=[step_spec(rows, channels)] * 2 + [whole_spec(1, channels)],
        out_shape=[
            jax.ShapeDtypeStruct((steps, rows, channels), F32),
            jax.ShapeDtypeStruct((steps, rows, channels), BF16),
            jax.ShapeDtypeStruct((1, channels), F32),
        ],
        compiler_params=PARAMS,
        name="middle",
    )(*attns, *projs, x, tgt)
    gbs = gather(gb)

    block_specs = [step_spec(rows, channels)] + [step_spec(*s) for s in block_shapes]
    dxns = []
    carry = ()
    for j in range(0, mp, 2):
        first, last = j == 0, j == mp - 2
        acc_type = BF16 if last else F32
        acc_shape = (channels, 4 * width) if last else (4 * width, channels)
        out = pl.pallas_call(
            functools.partial(backward_kernel, first, last, factor),
            grid=(steps,),
            in_specs=block_specs * 2
            + [whole_spec(width, channels), whole_spec(3, width, channels)]
            + ([] if first else [whole_spec(4 * width, channels), whole_spec(stacked, rows)]),
            out_specs=[step_spec(rows, channels)] * 2 + [whole_spec(*acc_shape), whole_spec(stacked, rows)],
            out_shape=[jax.ShapeDtypeStruct((steps, rows, channels), BF16)] * 2
            + [jax.ShapeDtypeStruct(acc_shape, acc_type), jax.ShapeDtypeStruct((stacked, rows), F32)],
            scratch_shapes=[pltpu.VMEM((4 * width, channels), F32)] if last else [],
            compiler_params=PARAMS,
            name="backward",
        )(gbs[j], *saved[j], gbs[j + 1], *saved[j + 1], w_proj, w_qkv, *carry)
        dxns += out[:2]
        carry = out[2:]
    weight_grads, table = carry

    parts = [dxns[0]] + [swap(dxns[k], k) for k in range(1, mp)]
    shard = channels // spread
    reduced = lax.psum_scatter(
        weight_grads.reshape(spread, shard, 4 * width), ("dp", "win"), scatter_dimension=0, tiled=False
    )

    table = table.reshape(heads, rows, rows)
    folded = table[:, :WIN_TOK, :WIN_TOK]
    for g in range(1, group):
        span = slice(g * WIN_TOK, (g + 1) * WIN_TOK)
        folded = folded + table[:, span, span]
    table_part = jnp.dot(folded.reshape(heads, -1), onehot, precision=lax.Precision.HIGHEST).T

    packed, gain_part = pl.pallas_call(
        functools.partial(final_kernel, mp),
        grid=(steps,),
        in_specs=[step_spec(rows, channels)] * (mp + 2) + [whole_spec(1, channels)],
        out_specs=[step_spec(rows, channels), whole_spec(1, channels)],
        out_shape=[
            jax.ShapeDtypeStruct((steps, rows, channels), F32),
            jax.ShapeDtypeStruct((1, channels), F32),
        ],
        compiler_params=PARAMS,
        name="final",
    )(*parts, x, gy, gain)
    input_gradient = packed[:, :valid].reshape(owned_rows, channels)

    grad_table = lax.psum(table_part, ("dp", "win")) * factor
    gain_gradient, total = lax.psum((gain_part[0], jnp.sum(squares)), ("dp", "win", "mp"))
    grads = reduced.astype(F32).T
    return (
        input_gradient,
        grads[: 3 * width].reshape(3, width, shard),
        grads[3 * width :],
        grad_table,
        gain_gradient * factor,
        0.5 * total / everyone,
    )


def solution(mesh):
    in_specs = (
        P(("dp", "win", "mp"), None),
        P(("dp", "win", "mp"), None),
        P(("dp", "win"), None),
        P(),
        P(),
        P(None, "mp"),
        P(None, "mp", None),
        P("mp", None),
    )
    out_specs = (
        P(("dp", "win", "mp"), None),
        P(None, "mp", ("dp", "win")),
        P("mp", ("dp", "win")),
        P(None, "mp"),
        P(),
        P(),
    )
    return jax.shard_map(
        per_device, mesh=mesh, in_specs=in_specs, out_specs=out_specs, check_vma=False
    )
```

```python
import functools

import jax
import jax.numpy as jnp
from jax import lax
from jax.experimental import pallas as pl
from jax.experimental.pallas import tpu as pltpu
from jax.sharding import PartitionSpec as P

HD = 32
WIN_TOK = 49
TABLE = 169
F32 = jnp.float32
BF16 = jnp.bfloat16
NEG = -1e30


def nt(a, b):
    return lax.dot_general(a, b, (((1,), (1,)), ((), ())), preferred_element_type=F32)


def nn(a, b):
    return lax.dot_general(a, b, (((1,), (0,)), ((), ())), preferred_element_type=F32)


def tn(a, b):
    return lax.dot_general(a, b, (((0,), (0,)), ((), ())), preferred_element_type=F32)


def head_masks(width, dtype):
    lane = lax.broadcasted_iota(jnp.int32, (1, width), 1) // HD
    return [(lane == h).astype(F32).astype(dtype) for h in range(width // HD)]


def stack_heads(a, masks):
    return jnp.concatenate([a * m for m in masks], axis=0)


def fold_heads(a, masks, rows):
    total = a[:rows] * masks[0]
    for h in range(1, len(masks)):
        total = total + a[h * rows : (h + 1) * rows] * masks[h]
    return total


def norm(x):
    width = x.shape[1]
    mean = jnp.sum(x, axis=1, keepdims=True) / width
    centered = x - mean
    var = jnp.sum(centered * centered, axis=1, keepdims=True) / width
    inv = lax.rsqrt(var + 1e-05)
    return centered * inv, inv


def forward_kernel(xa, xb, ma, mb, gain, w, relb, *outs):
    rows = xa.shape[1]
    width = w.shape[1]
    heads = width // HD
    x = jnp.concatenate([xa[0], xb[0]], axis=0).astype(F32)
    xhat, _ = norm(x)
    xn = (xhat * gain[...]).astype(BF16)
    q = (nt(xn, w[0]) * (HD**-0.5)).astype(BF16)
    k = nt(xn, w[1]).astype(BF16)
    v = nt(xn, w[2]).astype(BF16)
    mb16 = head_masks(width, BF16)
    mf32 = head_masks(width, F32)
    for i, mask in enumerate((ma, mb)):
        attn_out, q_out, k_out, v_out, p_out, xn_out = outs[6 * i : 6 * i + 6]
        span = slice(i * rows, (i + 1) * rows)
        qi, ki, vi = q[span], k[span], v[span]
        s = nt(stack_heads(qi, mb16), ki)
        s = (s + relb[...]).reshape(heads, rows, rows) + mask[...]
        s = s.reshape(heads * rows, rows)
        e = jnp.exp(s - jnp.max(s, axis=1, keepdims=True))
        probs = e * (1.0 / jnp.sum(e, axis=1, keepdims=True))
        o = nn(probs.astype(BF16), vi)
        attn_out[0] = fold_heads(o, mf32, rows).astype(BF16)
        q_out[0] = qi
        k_out[0] = ki
        v_out[0] = vi
        p_out[0] = probs
        xn_out[0] = xn[span]


def middle_kernel(count, valid, *refs):
    attns = refs[:count]
    projs = refs[count : 2 * count]
    x, target, gy_out, gb_out, sq_out = refs[2 * count :]
    total = jnp.zeros(x.shape[1:], F32)
    for a, w in zip(attns, projs):
        total = total + nn(a[0], w[...]).astype(BF16).astype(F32)
    gy = x[0].astype(F32) + total - target[0].astype(F32)
    row = lax.broadcasted_iota(jnp.int32, gy.shape, 0)
    gy = jnp.where(row < valid, gy, 0.0)
    gy_out[0] = gy
    gb_out[0] = gy.astype(BF16)

    @pl.when(pl.program_id(0) == 0)
    def _():
        sq_out[...] = jnp.zeros_like(sq_out)

    sq_out[...] += jnp.sum(gy * gy, axis=0, keepdims=True)


def backward_kernel(first, last, factor, *refs):
    ins = (refs[:7], refs[7:14])
    wp, w = refs[14:16]
    refs = refs[16:]
    if not first:
        acc_in, tab_in = refs[:2]
        refs = refs[2:]
    dxa, dxb, acc_out, tab_out = refs[:4]
    acc = refs[4] if last else acc_out
    width = w.shape[1]
    rows = dxa.shape[1]

    @pl.when(pl.program_id(0) == 0)
    def _():
        if first:
            acc[...] = jnp.zeros_like(acc)
            tab_out[...] = jnp.zeros_like(tab_out)
        else:
            acc[...] = acc_in[...]
            tab_out[...] = tab_in[...]

    mb16 = head_masks(width, BF16)
    mf32 = head_masks(width, F32)
    gb = jnp.concatenate([ins[0][0][0], ins[1][0][0]], axis=0)
    attn = jnp.concatenate([ins[0][1][0], ins[1][1][0]], axis=0)
    xn = jnp.concatenate([ins[0][6][0], ins[1][6][0]], axis=0)
    dattn = nt(gb, wp[...]).astype(BF16)
    parts = ([], [], [])
    table = tab_out[...]
    for i in range(2):
        _, _, q, k, v, p, _ = ins[i]
        das = stack_heads(dattn[i * rows : (i + 1) * rows], mb16)
        probs = p[0]
        pb = probs.astype(BF16)
        dprob = nt(das, v[0])
        ds = probs * (dprob - jnp.sum(probs * dprob, axis=1, keepdims=True))
        table = table + ds
        db = ds.astype(BF16)
        dq = fold_heads(nn(db, k[0]), mf32, rows) * (HD**-0.5)
        dk = tn(db, stack_heads(q[0], mb16))
        dv = tn(pb, das)
        for part, value in zip(parts, (dq, dk, dv)):
            part.append(value.astype(BF16))
    tab_out[...] = table
    grads = [jnp.concatenate(part, axis=0) for part in parts]
    dxn = nn(grads[0], w[0]) + nn(grads[1], w[1]) + nn(grads[2], w[2])
    dxa[0] = dxn[:rows].astype(BF16)
    dxb[0] = dxn[rows:].astype(BF16)
    for t in range(3):
        acc[t * width : (t + 1) * width] += tn(grads[t], xn)
    acc[3 * width :] += tn(attn, gb)
    if last:

        @pl.when(pl.program_id(0) == pl.num_programs(0) - 1)
        def _():
            acc_out[...] = (acc[...] * factor).T.astype(BF16)


def final_kernel(count, *refs):
    parts = refs[:count]
    x, gy, gain, out, gg_out = refs[count:]
    width = x.shape[2]
    xhat, inv = norm(x[0].astype(F32))
    dxn = parts[0][0].astype(F32)
    for part in parts[1:]:
        dxn = dxn + part[0].astype(F32)
    dxhat = dxn * gain[...]
    m1 = jnp.sum(dxhat, axis=1, keepdims=True) / width
    m2 = jnp.sum(dxhat * xhat, axis=1, keepdims=True) / width
    out[0] = gy[0] + inv * (dxhat - m1 - xhat * m2)

    @pl.when(pl.program_id(0) == 0)
    def _():
        gg_out[...] = jnp.zeros_like(gg_out)

    gg_out[...] += jnp.sum(dxn * xhat, axis=0, keepdims=True)


def step_spec(*shape):
    return pl.BlockSpec((1,) + shape, lambda p: (p,) + (0,) * len(shape))


def whole_spec(*shape):
    return pl.BlockSpec(shape, lambda p: (0,) * len(shape))


PARAMS = pltpu.CompilerParams(dimension_semantics=("arbitrary",))


def per_device(tokens, target, regions, rel_index, layer_norm_gain, bias_table, w_qkv, w_proj):
    owned_rows, channels = tokens.shape
    width = w_qkv.shape[1]
    heads = width // HD
    mp = lax.axis_size("mp")
    me = lax.axis_index("mp")
    spread = lax.axis_size("dp") * lax.axis_size("win")
    everyone = owned_rows * spread * mp
    factor = everyone ** (-0.5)
    owned_windows = owned_rows // WIN_TOK
    group = 2 if owned_windows % 2 == 0 else 1
    steps = owned_windows // group
    valid = group * WIN_TOK
    rows = -(-valid // 16) * 16
    stacked = heads * rows

    def pack(a):
        a = a.reshape(steps, valid, channels)
        return jnp.pad(a, ((0, 0), (0, rows - valid), (0, 0)))

    def swap(a, k):
        return lax.ppermute(a, "mp", [(i, i ^ k) for i in range(mp)])

    def far(a):
        return {k: swap(a, k) for k in range(2, mp, 2)}

    def near_pair(a, fars, j, done):
        if j == 0:
            return a, swap(a, 1)
        even, _ = lax.optimization_barrier((fars[j], done))
        return even, swap(even, 1)

    x = pack(tokens)
    tgt = pack(target)
    far_x = far(x)

    onehot = (rel_index.reshape(-1)[:, None] == jnp.arange(TABLE, dtype=jnp.int32)[None, :]).astype(F32)
    relbias = jnp.dot(onehot, bias_table, precision=lax.Precision.HIGHEST).T.reshape(heads, WIN_TOK, WIN_TOK)
    relb = jnp.zeros((heads, rows, rows), F32)
    for g in range(group):
        lo = g * WIN_TOK
        hi = rows - lo - WIN_TOK
        relb = relb + jnp.pad(relbias, ((0, 0), (lo, hi), (lo, hi)))
    relb = relb.reshape(stacked, rows)

    tags = regions.reshape(mp, steps, valid)
    tags = jnp.pad(tags, ((0, 0), (0, 0), (0, rows - valid)), constant_values=-1)
    spot = jnp.arange(rows, dtype=jnp.int32)
    near = (spot[:, None] // WIN_TOK == spot[None, :] // WIN_TOK) & (spot[None, :] < valid)
    maskv = jnp.where(tags[..., :, None] == tags[..., None, :], 0.0, -100.0)
    maskv = jnp.where(near, maskv, NEG).astype(F32)
    masks = [lax.dynamic_index_in_dim(maskv, me ^ k, 0, keepdims=False) for k in range(mp)]

    gain = layer_norm_gain[None, :]
    block_shapes = ((rows, width), (rows, width), (rows, width), (rows, width), (stacked, rows), (rows, channels))
    block_types = (BF16, BF16, BF16, BF16, F32, BF16)
    forward = pl.pallas_call(
        forward_kernel,
        grid=(steps,),
        in_specs=[step_spec(rows, channels)] * 2
        + [step_spec(rows, rows)] * 2
        + [whole_spec(1, channels), whole_spec(3, width, channels), whole_spec(stacked, rows)],
        out_specs=[step_spec(*s) for s in block_shapes] * 2,
        out_shape=[jax.ShapeDtypeStruct((steps,) + s, t) for s, t in zip(block_shapes, block_types)] * 2,
        compiler_params=PARAMS,
        name="forward",
    )
    saved = []
    done = None
    for j in range(0, mp, 2):
        xa, xb = near_pair(x, far_x, j, done)
        res = forward(xa, xb, masks[j], masks[j + 1], gain, w_qkv, relb)
        saved += [res[:6], res[6:]]
        done = res[0]
        if j == 0:
            tied, _ = lax.optimization_barrier((w_proj, done))
            far_w = far(tied)
            projs = list(near_pair(tied, far_w, 0, None))
    for j in range(2, mp, 2):
        projs += [far_w[j], swap(far_w[j], 1)]

    attns = [saved[0][0]] + [swap(saved[k][0], k) for k in range(1, mp)]
    gy, gb, squares = pl.pallas_call(
        functools.partial(middle_kernel, mp, valid),
        grid=(steps,),
        in_specs=[step_spec(rows, width)] * mp
        + [whole_spec(width, channels)] * mp
        + [step_spec(rows, channels)] * 2,
        out_specs=[step_spec(rows, channels)] * 2 + [whole_spec(1, channels)],
        out_shape=[
            jax.ShapeDtypeStruct((steps, rows, channels), F32),
            jax.ShapeDtypeStruct((steps, rows, channels), BF16),
            jax.ShapeDtypeStruct((1, channels), F32),
        ],
        compiler_params=PARAMS,
        name="middle",
    )(*attns, *projs, x, tgt)
    far_gb = far(gb)

    block_specs = [step_spec(rows, channels)] + [step_spec(*s) for s in block_shapes]
    dxns = []
    carry = ()
    for j in range(0, mp, 2):
        ga, gb2 = near_pair(gb, far_gb, j, dxns[0] if j else None)
        first, last = j == 0, j == mp - 2
        acc_type = BF16 if last else F32
        acc_shape = (channels, 4 * width) if last else (4 * width, channels)
        out = pl.pallas_call(
            functools.partial(backward_kernel, first, last, factor),
            grid=(steps,),
            in_specs=block_specs * 2
            + [whole_spec(width, channels), whole_spec(3, width, channels)]
            + ([] if first else [whole_spec(4 * width, channels), whole_spec(stacked, rows)]),
            out_specs=[step_spec(rows, channels)] * 2 + [whole_spec(*acc_shape), whole_spec(stacked, rows)],
            out_shape=[jax.ShapeDtypeStruct((steps, rows, channels), BF16)] * 2
            + [jax.ShapeDtypeStruct(acc_shape, acc_type), jax.ShapeDtypeStruct((stacked, rows), F32)],
            scratch_shapes=[pltpu.VMEM((4 * width, channels), F32)] if last else [],
            compiler_params=PARAMS,
            name="backward",
        )(ga, *saved[j], gb2, *saved[j + 1], w_proj, w_qkv, *carry)
        dxns += out[:2]
        carry = out[2:]
    weight_grads, table = carry

    parts = [dxns[0], swap(dxns[1], 1)]
    for k in range(2, mp, 2):
        both = dxns[k].astype(F32) + swap(dxns[k + 1], 1).astype(F32)
        parts.append(swap(both.astype(BF16), k))

    def send(a, axis):
        size = lax.axis_size(axis)
        here = lax.axis_index(axis)

        def piece(k):
            return lax.dynamic_index_in_dim(a, here ^ k, 0, keepdims=False)

        return [piece(0)] + [
            lax.ppermute(piece(k), axis, [(i, i ^ k) for i in range(size)]) for k in range(1, size)
        ]

    def add(values):
        total = values[0].astype(F32)
        for value in values[1:]:
            total = total + value.astype(F32)
        return total

    shard = channels // spread
    grid = weight_grads.reshape(lax.axis_size("dp"), lax.axis_size("win"), shard, 4 * width)
    halfway = add(send(grid.transpose(1, 0, 2, 3), "win")).astype(BF16)
    shares = send(halfway, "dp")

    table = table.reshape(heads, rows, rows)
    folded = table[:, :WIN_TOK, :WIN_TOK]
    for g in range(1, group):
        span = slice(g * WIN_TOK, (g + 1) * WIN_TOK)
        folded = folded + table[:, span, span]
    table_part = jnp.dot(folded.reshape(heads, -1), onehot, precision=lax.Precision.HIGHEST).T

    packed, gain_part = pl.pallas_call(
        functools.partial(final_kernel, len(parts)),
        grid=(steps,),
        in_specs=[step_spec(rows, channels)] * (len(parts) + 2) + [whole_spec(1, channels)],
        out_specs=[step_spec(rows, channels), whole_spec(1, channels)],
        out_shape=[
            jax.ShapeDtypeStruct((steps, rows, channels), F32),
            jax.ShapeDtypeStruct((1, channels), F32),
        ],
        compiler_params=PARAMS,
        name="final",
    )(*parts, x, gy, gain)
    input_gradient = packed[:, :valid].reshape(owned_rows, channels)

    mine = (jnp.arange(mp) == me).astype(F32)
    tables = mine[:, None, None] * table_part[None]
    small = jnp.concatenate([tables.reshape(-1), gain_part[0], jnp.sum(squares)[None]])
    small, _ = lax.optimization_barrier((small, halfway))
    small = lax.psum(small, ("dp", "win", "mp"))
    tables = small[: tables.size].reshape(tables.shape)
    grad_table = lax.dynamic_index_in_dim(tables, me, 0, keepdims=False) * factor
    gain_gradient, total = small[tables.size : -1], small[-1]
    shares, _ = lax.optimization_barrier((shares, small))
    grads = add(shares).T
    return (
        input_gradient,
        grads[: 3 * width].reshape(3, width, shard),
        grads[3 * width :],
        grad_table,
        gain_gradient * factor,
        0.5 * total / everyone,
    )


def solution(mesh):
    in_specs = (
        P(("dp", "win", "mp"), None),
        P(("dp", "win", "mp"), None),
        P(("dp", "win"), None),
        P(),
        P(),
        P(None, "mp"),
        P(None, "mp", None),
        P("mp", None),
    )
    out_specs = (
        P(("dp", "win", "mp"), None),
        P(None, "mp", ("dp", "win")),
        P("mp", ("dp", "win")),
        P(None, "mp"),
        P(),
        P(),
    )
    return jax.shard_map(
        per_device, mesh=mesh, in_specs=in_specs, out_specs=out_specs, check_vma=False
    )
```

```python
import functools

import jax
import jax.numpy as jnp
from jax import lax
from jax.experimental import pallas as pl
from jax.experimental.pallas import tpu as pltpu
from jax.sharding import PartitionSpec as P

HD = 32
WIN_TOK = 49
TABLE = 169
F32 = jnp.float32
BF16 = jnp.bfloat16
NEG = -1e30


def nt(a, b):
    return lax.dot_general(a, b, (((1,), (1,)), ((), ())), preferred_element_type=F32)


def nn(a, b):
    return lax.dot_general(a, b, (((1,), (0,)), ((), ())), preferred_element_type=F32)


def tn(a, b):
    return lax.dot_general(a, b, (((0,), (0,)), ((), ())), preferred_element_type=F32)


def head_masks(width, dtype):
    lane = lax.broadcasted_iota(jnp.int32, (1, width), 1) // HD
    return [(lane == h).astype(F32).astype(dtype) for h in range(width // HD)]


def stack_heads(a, masks):
    return jnp.concatenate([a * m for m in masks], axis=0)


def fold_heads(a, masks, rows):
    total = a[:rows] * masks[0]
    for h in range(1, len(masks)):
        total = total + a[h * rows : (h + 1) * rows] * masks[h]
    return total


def norm(x):
    width = x.shape[1]
    mean = jnp.sum(x, axis=1, keepdims=True) / width
    centered = x - mean
    var = jnp.sum(centered * centered, axis=1, keepdims=True) / width
    inv = lax.rsqrt(var + 1e-05)
    return centered * inv, inv


def forward_kernel(xa, xb, ma, mb, gain, w, relb, *outs):
    rows = xa.shape[1]
    width = w.shape[1]
    heads = width // HD
    x = jnp.concatenate([xa[0], xb[0]], axis=0).astype(F32)
    xhat, _ = norm(x)
    xn = (xhat * gain[...]).astype(BF16)
    q = (nt(xn, w[0]) * (HD**-0.5)).astype(BF16)
    k = nt(xn, w[1]).astype(BF16)
    v = nt(xn, w[2]).astype(BF16)
    mb16 = head_masks(width, BF16)
    mf32 = head_masks(width, F32)
    for i, mask in enumerate((ma, mb)):
        attn_out, q_out, k_out, v_out, p_out, xn_out = outs[6 * i : 6 * i + 6]
        span = slice(i * rows, (i + 1) * rows)
        qi, ki, vi = q[span], k[span], v[span]
        s = nt(stack_heads(qi, mb16), ki)
        s = (s + relb[...]).reshape(heads, rows, rows) + mask[...]
        s = s.reshape(heads * rows, rows)
        e = jnp.exp(s - jnp.max(s, axis=1, keepdims=True))
        probs = e * (1.0 / jnp.sum(e, axis=1, keepdims=True))
        o = nn(probs.astype(BF16), vi)
        attn_out[0] = fold_heads(o, mf32, rows).astype(BF16)
        q_out[0] = qi
        k_out[0] = ki
        v_out[0] = vi
        p_out[0] = probs
        xn_out[0] = xn[span]


def middle_kernel(count, valid, *refs):
    attns = refs[:count]
    projs = refs[count : 2 * count]
    x, target, gy_out, gb_out, sq_out = refs[2 * count :]
    total = jnp.zeros(x.shape[1:], F32)
    for a, w in zip(attns, projs):
        total = total + nn(a[0], w[...]).astype(BF16).astype(F32)
    gy = x[0].astype(F32) + total - target[0].astype(F32)
    row = lax.broadcasted_iota(jnp.int32, gy.shape, 0)
    gy = jnp.where(row < valid, gy, 0.0)
    gy_out[0] = gy
    gb_out[0] = gy.astype(BF16)

    @pl.when(pl.program_id(0) == 0)
    def _():
        sq_out[...] = jnp.zeros_like(sq_out)

    sq_out[...] += jnp.sum(gy * gy, axis=0, keepdims=True)


def backward_kernel(first, last, factor, *refs):
    ins = (refs[:7], refs[7:14])
    wp, w = refs[14:16]
    refs = refs[16:]
    if not first:
        acc_in, tab_in = refs[:2]
        refs = refs[2:]
    dxa, dxb, acc_out, tab_out = refs[:4]
    acc = refs[4] if last else acc_out
    width = w.shape[1]
    rows = dxa.shape[1]

    @pl.when(pl.program_id(0) == 0)
    def _():
        if first:
            acc[...] = jnp.zeros_like(acc)
            tab_out[...] = jnp.zeros_like(tab_out)
        else:
            acc[...] = acc_in[...]
            tab_out[...] = tab_in[...]

    mb16 = head_masks(width, BF16)
    mf32 = head_masks(width, F32)
    gb = jnp.concatenate([ins[0][0][0], ins[1][0][0]], axis=0)
    attn = jnp.concatenate([ins[0][1][0], ins[1][1][0]], axis=0)
    xn = jnp.concatenate([ins[0][6][0], ins[1][6][0]], axis=0)
    dattn = nt(gb, wp[...]).astype(BF16)
    parts = ([], [], [])
    table = tab_out[...]
    for i in range(2):
        _, _, q, k, v, p, _ = ins[i]
        das = stack_heads(dattn[i * rows : (i + 1) * rows], mb16)
        probs = p[0]
        pb = probs.astype(BF16)
        dprob = nt(das, v[0])
        ds = probs * (dprob - jnp.sum(probs * dprob, axis=1, keepdims=True))
        table = table + ds
        db = ds.astype(BF16)
        dq = fold_heads(nn(db, k[0]), mf32, rows) * (HD**-0.5)
        dk = tn(db, stack_heads(q[0], mb16))
        dv = tn(pb, das)
        for part, value in zip(parts, (dq, dk, dv)):
            part.append(value.astype(BF16))
    tab_out[...] = table
    grads = [jnp.concatenate(part, axis=0) for part in parts]
    dxn = nn(grads[0], w[0]) + nn(grads[1], w[1]) + nn(grads[2], w[2])
    dxa[0] = dxn[:rows].astype(BF16)
    dxb[0] = dxn[rows:].astype(BF16)
    for t in range(3):
        acc[t * width : (t + 1) * width] += tn(grads[t], xn)
    acc[3 * width :] += tn(attn, gb)
    if last:

        @pl.when(pl.program_id(0) == pl.num_programs(0) - 1)
        def _():
            acc_out[...] = (acc[...] * factor).T.astype(BF16)


def final_kernel(count, *refs):
    parts = refs[:count]
    x, gy, gain, out, gg_out = refs[count:]
    width = x.shape[2]
    xhat, inv = norm(x[0].astype(F32))
    dxn = parts[0][0].astype(F32)
    for part in parts[1:]:
        dxn = dxn + part[0].astype(F32)
    dxhat = dxn * gain[...]
    m1 = jnp.sum(dxhat, axis=1, keepdims=True) / width
    m2 = jnp.sum(dxhat * xhat, axis=1, keepdims=True) / width
    out[0] = gy[0] + inv * (dxhat - m1 - xhat * m2)

    @pl.when(pl.program_id(0) == 0)
    def _():
        gg_out[...] = jnp.zeros_like(gg_out)

    gg_out[...] += jnp.sum(dxn * xhat, axis=0, keepdims=True)


def step_spec(*shape):
    return pl.BlockSpec((1,) + shape, lambda p: (p,) + (0,) * len(shape))


def whole_spec(*shape):
    return pl.BlockSpec(shape, lambda p: (0,) * len(shape))


PARAMS = pltpu.CompilerParams(dimension_semantics=("arbitrary",))


def per_device(tokens, target, regions, rel_index, layer_norm_gain, bias_table, w_qkv, w_proj):
    owned_rows, channels = tokens.shape
    width = w_qkv.shape[1]
    heads = width // HD
    mp = lax.axis_size("mp")
    me = lax.axis_index("mp")
    spread = lax.axis_size("dp") * lax.axis_size("win")
    everyone = owned_rows * spread * mp
    factor = everyone ** (-0.5)
    owned_windows = owned_rows // WIN_TOK
    group = 2 if owned_windows % 2 == 0 else 1
    steps = owned_windows // group
    valid = group * WIN_TOK
    rows = -(-valid // 16) * 16
    stacked = heads * rows

    def pack(a):
        a = a.reshape(steps, valid, channels)
        return jnp.pad(a, ((0, 0), (0, rows - valid), (0, 0)))

    def swap(a, k):
        return lax.ppermute(a, "mp", [(i, i ^ k) for i in range(mp)])

    def far(a):
        return {k: swap(a, k) for k in range(2, mp, 2)}

    def near_pair(a, fars, j, done):
        if j == 0:
            return a, swap(a, 1)
        even, _ = lax.optimization_barrier((fars[j], done))
        return even, swap(even, 1)

    x = pack(tokens)
    tgt = pack(target)
    far_x = far(x)

    onehot = (rel_index.reshape(-1)[:, None] == jnp.arange(TABLE, dtype=jnp.int32)[None, :]).astype(F32)
    relbias = jnp.dot(onehot, bias_table, precision=lax.Precision.HIGHEST).T.reshape(heads, WIN_TOK, WIN_TOK)
    relb = jnp.zeros((heads, rows, rows), F32)
    for g in range(group):
        lo = g * WIN_TOK
        hi = rows - lo - WIN_TOK
        relb = relb + jnp.pad(relbias, ((0, 0), (lo, hi), (lo, hi)))
    relb = relb.reshape(stacked, rows)

    tags = regions.reshape(mp, steps, valid)
    tags = jnp.pad(tags, ((0, 0), (0, 0), (0, rows - valid)), constant_values=-1)
    spot = jnp.arange(rows, dtype=jnp.int32)
    near = (spot[:, None] // WIN_TOK == spot[None, :] // WIN_TOK) & (spot[None, :] < valid)
    maskv = jnp.where(tags[..., :, None] == tags[..., None, :], 0.0, -100.0)
    maskv = jnp.where(near, maskv, NEG).astype(F32)
    masks = [lax.dynamic_index_in_dim(maskv, me ^ k, 0, keepdims=False) for k in range(mp)]

    gain = layer_norm_gain[None, :]
    block_shapes = ((rows, width), (rows, width), (rows, width), (rows, width), (stacked, rows), (rows, channels))
    block_types = (BF16, BF16, BF16, BF16, F32, BF16)
    forward = pl.pallas_call(
        forward_kernel,
        grid=(steps,),
        in_specs=[step_spec(rows, channels)] * 2
        + [step_spec(rows, rows)] * 2
        + [whole_spec(1, channels), whole_spec(3, width, channels), whole_spec(stacked, rows)],
        out_specs=[step_spec(*s) for s in block_shapes] * 2,
        out_shape=[jax.ShapeDtypeStruct((steps,) + s, t) for s, t in zip(block_shapes, block_types)] * 2,
        compiler_params=PARAMS,
        name="forward",
    )
    saved = []
    done = None
    for j in range(0, mp, 2):
        xa, xb = near_pair(x, far_x, j, done)
        res = forward(xa, xb, masks[j], masks[j + 1], gain, w_qkv, relb)
        saved += [res[:6], res[6:]]
        done = res[0]
        if j == 0:
            tied, _ = lax.optimization_barrier((w_proj, done))
            far_w = far(tied)
            projs = list(near_pair(tied, far_w, 0, None))
    for j in range(2, mp, 2):
        projs += [far_w[j], swap(far_w[j], 1)]

    attns = [saved[0][0]] + [swap(saved[k][0], k) for k in range(1, mp)]
    gy, gb, squares = pl.pallas_call(
        functools.partial(middle_kernel, mp, valid),
        grid=(steps,),
        in_specs=[step_spec(rows, width)] * mp
        + [whole_spec(width, channels)] * mp
        + [step_spec(rows, channels)] * 2,
        out_specs=[step_spec(rows, channels)] * 2 + [whole_spec(1, channels)],
        out_shape=[
            jax.ShapeDtypeStruct((steps, rows, channels), F32),
            jax.ShapeDtypeStruct((steps, rows, channels), BF16),
            jax.ShapeDtypeStruct((1, channels), F32),
        ],
        compiler_params=PARAMS,
        name="middle",
    )(*attns, *projs, x, tgt)
    far_gb = far(gb)

    block_specs = [step_spec(rows, channels)] + [step_spec(*s) for s in block_shapes]
    dxns = []
    carry = ()
    for j in range(0, mp, 2):
        ga, gb2 = near_pair(gb, far_gb, j, dxns[0] if j else None)
        first, last = j == 0, j == mp - 2
        acc_type = BF16 if last else F32
        acc_shape = (channels, 4 * width) if last else (4 * width, channels)
        out = pl.pallas_call(
            functools.partial(backward_kernel, first, last, factor),
            grid=(steps,),
            in_specs=block_specs * 2
            + [whole_spec(width, channels), whole_spec(3, width, channels)]
            + ([] if first else [whole_spec(4 * width, channels), whole_spec(stacked, rows)]),
            out_specs=[step_spec(rows, channels)] * 2 + [whole_spec(*acc_shape), whole_spec(stacked, rows)],
            out_shape=[jax.ShapeDtypeStruct((steps, rows, channels), BF16)] * 2
            + [jax.ShapeDtypeStruct(acc_shape, acc_type), jax.ShapeDtypeStruct((stacked, rows), F32)],
            scratch_shapes=[pltpu.VMEM((4 * width, channels), F32)] if last else [],
            compiler_params=PARAMS,
            name="backward",
        )(ga, *saved[j], gb2, *saved[j + 1], w_proj, w_qkv, *carry)
        dxns += out[:2]
        carry = out[2:]
    weight_grads, table = carry

    parts = [dxns[0], swap(dxns[1], 1)]
    for k in range(2, mp, 2):
        both = dxns[k].astype(F32) + swap(dxns[k + 1], 1).astype(F32)
        parts.append(swap(both.astype(BF16), k))

    def send(a, axis):
        size = lax.axis_size(axis)
        here = lax.axis_index(axis)

        def piece(k):
            return lax.dynamic_index_in_dim(a, here ^ k, 0, keepdims=False)

        return [piece(0)] + [
            lax.ppermute(piece(k), axis, [(i, i ^ k) for i in range(size)]) for k in range(1, size)
        ]

    def add(values):
        total = values[0].astype(F32)
        for value in values[1:]:
            total = total + value.astype(F32)
        return total

    shard = channels // spread
    grid = weight_grads.reshape(lax.axis_size("dp"), lax.axis_size("win"), shard, 4 * width)
    halfway = add(send(grid.transpose(1, 0, 2, 3), "win")).astype(BF16)
    shares = send(halfway, "dp")

    table = table.reshape(heads, rows, rows)
    folded = table[:, :WIN_TOK, :WIN_TOK]
    for g in range(1, group):
        span = slice(g * WIN_TOK, (g + 1) * WIN_TOK)
        folded = folded + table[:, span, span]
    table_part = jnp.dot(folded.reshape(heads, -1), onehot, precision=lax.Precision.HIGHEST).T

    packed, gain_part = pl.pallas_call(
        functools.partial(final_kernel, len(parts)),
        grid=(steps,),
        in_specs=[step_spec(rows, channels)] * (len(parts) + 2) + [whole_spec(1, channels)],
        out_specs=[step_spec(rows, channels), whole_spec(1, channels)],
        out_shape=[
            jax.ShapeDtypeStruct((steps, rows, channels), F32),
            jax.ShapeDtypeStruct((1, channels), F32),
        ],
        compiler_params=PARAMS,
        name="final",
    )(*parts, x, gy, gain)
    input_gradient = packed[:, :valid].reshape(owned_rows, channels)

    def everywhere(a, axis):
        size = lax.axis_size(axis)
        values = [a] + [lax.ppermute(a, axis, [(i, i ^ k) for i in range(size)]) for k in range(1, size)]
        while len(values) > 1:
            values = [l + r for l, r in zip(values[::2], values[1::2])]
        return values[0]

    table_sum = everywhere(everywhere(table_part.reshape(-1), "win"), "dp")
    grad_table = table_sum.reshape(table_part.shape) * factor
    small = jnp.concatenate([gain_part[0], jnp.sum(squares)[None]])
    small, _ = lax.optimization_barrier((small, halfway))
    for axis in ("mp", "win", "dp"):
        small = everywhere(small, axis)
    gain_gradient, total = small[:-1], small[-1]
    shares, _ = lax.optimization_barrier((shares, small))
    grads = add(shares).T
    return (
        input_gradient,
        grads[: 3 * width].reshape(3, width, shard),
        grads[3 * width :],
        grad_table,
        gain_gradient * factor,
        0.5 * total / everyone,
    )


def solution(mesh):
    in_specs = (
        P(("dp", "win", "mp"), None),
        P(("dp", "win", "mp"), None),
        P(("dp", "win"), None),
        P(),
        P(),
        P(None, "mp"),
        P(None, "mp", None),
        P("mp", None),
    )
    out_specs = (
        P(("dp", "win", "mp"), None),
        P(None, "mp", ("dp", "win")),
        P("mp", ("dp", "win")),
        P(None, "mp"),
        P(),
        P(),
    )
    return jax.shard_map(
        per_device, mesh=mesh, in_specs=in_specs, out_specs=out_specs, check_vma=False
    )
```
